256 devices in a mesh: rows: 128 (over z, x, y), feat: 2 (over core).
Axes of the slice: x: 4, y: 4, z: 8, core: 2. Of those that a mesh axis runs over, the one named last changes fastest.
Arguments:
- score: float32 [262144, 128], P('rows', 'feat'), may hold values from -4 to 4
- event: int32 [262144, 128], P('rows', 'feat'), may hold values 0 or 1
- leaf: int32 [262144, 128], P('rows', 'feat'), may hold values from 0 to 1
- bins: int32 [262144, 256], P('rows'), may hold values from 0 to 31
- split_feature: int32 [128], P('feat'), may hold values from 0 to 255
- split_bin: int32 [128], P('feat'), may hold values from 0 to 30
Outputs:
- grad_hist: float32 [256, 32, 2, 128], P(('rows', 'feat'))
- hess_hist: float32 [256, 32, 2, 128], P(('rows', 'feat'))
- new_leaf: int32 [262144, 128], P('rows', 'feat')
The draws below stay inside these ranges and needn't reach their ends.
All inputs are finite; a program needn't handle non-finite values. No bound on the sum of `event` on one device may be relied on, other than what follows from the above.
Results may differ from the reference program's by a relative error of at most 0.0026.
Values may be sent and summed in bfloat16 or wider, within the bound.
No kernel may reach another device: no remote copies, remote signals or barrier semaphores. Data moves between devices by JAX's collectives and lax.ppermute only.
A program may use at most 64 MiB of HBM per device.

```python
import jax
import jax.numpy as jnp
from jax import lax

ENDPOINTS = 128
FEATURES = 256
BINS = 32
LEAVES = 2
SAMPLES = 262144


def draw_score(key, part):
    key_noise = jax.random.fold_in(jax.random.fold_in(key, 7), 0)
    position = jnp.arange(SAMPLES, dtype=jnp.float32)[:, None] / SAMPLES
    jitter = 0.7 * jax.random.normal(key_noise, (SAMPLES, ENDPOINTS), jnp.float32)
    trend_rate = 1.1 * jnp.ones((1, ENDPOINTS), jnp.float32)
    return jnp.clip(jitter + trend_rate * (position - 0.5), -4.0, 4.0)


def set_ends(entries, rng, low, largest):
    longest = entries.shape.index(max(entries.shape))
    spots = []
    for shift in (0, 1):
        where = [jax.random.randint(jax.random.fold_in(rng, axis), (), 0, length) for axis, length in enumerate(entries.shape)]
        where[longest] = (where[longest] + shift) % entries.shape[longest]
        spots.append(tuple(where))
    return entries.at[spots[0]].set(low).at[spots[1]].set(largest)


def setup_inputs(seed: int = 0) -> dict:
    key_list = jax.random.split(jax.random.key(seed), 7)
    score = draw_score(jax.random.fold_in(key_list[6], 71), 0)
    event = set_ends((jax.random.randint(key_list[1], (SAMPLES, ENDPOINTS), 0, 4) < 1).astype(jnp.int32), jax.random.fold_in(key_list[1], 1), 0, 1)
    leaf = set_ends(jax.random.randint(key_list[2], (SAMPLES, ENDPOINTS), 0, LEAVES), jax.random.fold_in(key_list[2], 1), 0, LEAVES - 1).astype(jnp.int32)
    bins = set_ends(jax.random.randint(key_list[3], (SAMPLES, FEATURES), 0, BINS), jax.random.fold_in(key_list[3], 1), 0, BINS - 1).astype(jnp.int32)
    split_feature = set_ends(jax.random.randint(key_list[4], (ENDPOINTS,), 0, FEATURES), jax.random.fold_in(key_list[4], 1), 0, FEATURES - 1).astype(jnp.int32)
    split_bin = set_ends(jax.random.randint(key_list[5], (ENDPOINTS,), 0, BINS - 1), jax.random.fold_in(key_list[5], 1), 0, (BINS - 1) - 1).astype(jnp.int32)
    return {"score": score, "event": event, "leaf": leaf, "bins": bins, "split_feature": split_feature, "split_bin": split_bin}


def reference(score, event, leaf, bins, split_feature, split_bin):
    exp_score = jnp.exp(score)
    risk_sum = jnp.cumsum(exp_score[::-1], axis=0)[::-1]
    event_mass = event.astype(jnp.float32)
    event_share = event_mass / risk_sum
    cum_hazard = jnp.cumsum(event_share, axis=0)
    cum_square = jnp.cumsum(event_share / risk_sum, axis=0)
    scale_factor = BINS * LEAVES / SAMPLES
    gradient = scale_factor * (exp_score * cum_hazard - event_mass)
    hessian = scale_factor * (exp_score * cum_hazard - exp_score * exp_score * cum_square)
    in_leaf = leaf[:, None, :] == jnp.arange(LEAVES, dtype=jnp.int32)[None, :, None]
    leaf_weights = jnp.stack([jnp.where(in_leaf, gradient[:, None, :], jnp.zeros((), jnp.float32)),
                              jnp.where(in_leaf, hessian[:, None, :], jnp.zeros((), jnp.float32))], axis=1).astype(jnp.bfloat16)
    flat_weights = leaf_weights.reshape(SAMPLES, 2 * LEAVES * ENDPOINTS).astype(jnp.float32)

    def feature_hist(column):
        return jax.ops.segment_sum(flat_weights, column, num_segments=BINS)

    histograms = lax.map(feature_hist, bins.T).reshape(FEATURES, BINS, 2, LEAVES, ENDPOINTS)
    split_value = jnp.take(bins, split_feature, axis=1)
    new_leaf = 2 * leaf + (split_value > split_bin[None, :]).astype(jnp.int32)
    return histograms[:, :, 0], histograms[:, :, 1], new_leaf
```

```python
import jax
import jax.numpy as jnp
from jax import lax
from jax.experimental import pallas as pl
from jax.experimental.pallas import tpu as pltpu
from jax.sharding import Mesh
from jax.sharding import PartitionSpec as P

BINS = 32
LEAVES = 2
ROWS = ("rows_0", "rows_1", "rows_2")
PLANE = ("rows_1", "rows_2")
DEPTH_FEAT = ("rows_0", "feat")
ROWS_FEAT = ("rows_0", "rows_1", "rows_2", "feat")
BLOCK = 256
HIGHEST = lax.Precision.HIGHEST
F32 = jnp.float32
DOWN = 2.0**-3


def swap(x, axis):
    return lax.all_to_all(x, axis, split_axis=0, concat_axis=0, tiled=True)


def peers_sum(x, earlier):
    planes = lax.axis_size("rows_0")
    members = lax.axis_size(PLANE)
    here = lax.axis_index(PLANE)
    plane = lax.axis_index("rows_0")
    got = swap(jnp.broadcast_to(x[None], (members, x.shape[0])), PLANE)
    index = lax.broadcasted_iota(jnp.int32, (members, 1), 0)
    chosen = (index < here) if earlier else (index > here)
    inside = jnp.sum(jnp.where(chosen, got, 0.0), axis=0)
    total = jnp.sum(got, axis=0)
    got = swap(jnp.broadcast_to(total[None], (planes, x.shape[0])), "rows_0")
    index = lax.broadcasted_iota(jnp.int32, (planes, 1), 0)
    chosen = (index < plane) if earlier else (index > plane)
    return inside + jnp.sum(jnp.where(chosen, got, 0.0), axis=0)


def as_column(line):
    n = line.shape[1]
    row = lax.broadcasted_iota(jnp.int32, (n, n), 0)
    col = lax.broadcasted_iota(jnp.int32, (n, n), 1)
    return jnp.sum(jnp.where(row == col, jnp.broadcast_to(line, (n, n)), 0.0), axis=1, keepdims=True)


def as_line(column):
    n = column.shape[0]
    row = lax.broadcasted_iota(jnp.int32, (n, n), 0)
    col = lax.broadcasted_iota(jnp.int32, (n, n), 1)
    return jnp.sum(jnp.where(row == col, jnp.broadcast_to(column, (n, n)), 0.0), axis=0, keepdims=True)


def prefix_kernel(score_ref, event_ref, later_ref, local_ref, total_ref):
    width, rows = score_ref.shape
    row = lax.broadcasted_iota(jnp.int32, (BLOCK, BLOCK), 0)
    col = lax.broadcasted_iota(jnp.int32, (BLOCK, BLOCK), 1)
    suffix = (row >= col).astype(F32)
    prefix = (row <= col).astype(F32)
    blocks = rows // BLOCK
    runs = [
        lax.dot(
            jnp.exp(score_ref[:, pl.ds(k * BLOCK, BLOCK)]),
            suffix,
            precision=HIGHEST,
            preferred_element_type=F32,
        )
        for k in range(blocks)
    ]
    carry = as_column(later_ref[...])
    both = [None] * blocks
    for k in reversed(range(blocks)):
        inverse = 1.0 / (runs[k] + carry)
        carry = carry + runs[k][:, :1]
        share = event_ref[:, pl.ds(k * BLOCK, BLOCK)].astype(F32) * inverse
        both[k] = jnp.concatenate([share, share * inverse], axis=0)
    runs = [
        lax.dot(both[k], prefix, precision=HIGHEST, preferred_element_type=F32)
        for k in range(blocks)
    ]
    carry = jnp.zeros((2 * width, 1), F32)
    for k in range(blocks):
        local_ref[:, pl.ds(k * BLOCK, BLOCK)] = runs[k] + carry
        carry = carry + runs[k][:, BLOCK - 1 :]
    total_ref[...] = as_line(carry)


def hist_kernel(score_ref, event_ref, leaf_ref, local_ref, base_ref, bins_ref, out_ref, w_ref):
    width, rows = score_ref.shape
    feats = bins_ref.shape[0]

    @pl.when(pl.program_id(0) == 0)
    def _():
        base = as_column(base_ref[...])
        for k in range(rows // BLOCK):
            at = pl.ds(k * BLOCK, BLOCK)
            e = jnp.exp(score_ref[:, at])
            first = e * (local_ref[:width, at] + base[:width])
            second = e * e * (local_ref[width:, at] + base[width:])
            g = (first - event_ref[:, at].astype(F32)) * DOWN
            h = (first - second) * DOWN
            leaf = leaf_ref[:, at]
            for n, v in enumerate((g, h)):
                for m in range(LEAVES):
                    w_ref[pl.ds((n * LEAVES + m) * width, width), at] = jnp.where(
                        leaf == m, v, 0.0
                    ).astype(jnp.bfloat16)

    group = 8
    level = lax.broadcasted_iota(jnp.int32, (BINS, rows), 0).astype(F32).astype(jnp.bfloat16)
    one = jnp.ones((), jnp.bfloat16)
    zero = jnp.zeros((), jnp.bfloat16)
    for j in range(feats // group):
        tiles = []
        for i in range(group):
            line = bins_ref[pl.ds(j * group + i, 1), :]
            line = jnp.broadcast_to(line, (BINS, rows)).astype(jnp.bfloat16)
            tiles.append(jnp.where(line == level, one, zero))
        hot = jnp.concatenate(tiles, axis=0)
        got = lax.dot_general(
            hot, w_ref[...], (((1,), (1,)), ((), ())), preferred_element_type=F32
        )
        per = out_ref.shape[2]
        n = group * BINS // per
        out_ref[pl.ds(j * n, n), 0] = got.reshape(n, per, got.shape[1])


def per_device(score, event, leaf, bins, split_feature, split_bin):
    rows, width = score.shape
    feats = bins.shape[1]
    shards = lax.axis_size(ROWS)
    planes = lax.axis_size("rows_0")
    members = lax.axis_size(PLANE)
    cores = lax.axis_size("feat")
    cols = 2 * LEAVES * width
    total = jnp.sum(jnp.exp(score), axis=0)
    later = peers_sum(total, False)
    local, sums = pl.pallas_call(
        prefix_kernel,
        out_shape=(
            jax.ShapeDtypeStruct((2 * width, rows), F32),
            jax.ShapeDtypeStruct((1, 2 * width), F32),
        ),
    )(score.T, event.T, later[None])
    base = peers_sum(sums[0], True)
    columns = bins.T.astype(F32)
    slab = feats // planes
    own = BINS * feats // shards
    whole = lambda *shape: pl.BlockSpec(shape, lambda z: (0,) * len(shape))
    parts = pl.pallas_call(
        hist_kernel,
        grid=(planes,),
        in_specs=[
            whole(width, rows),
            whole(width, rows),
            whole(width, rows),
            whole(2 * width, rows),
            whole(1, 2 * width),
            pl.BlockSpec((slab, rows), lambda z: (z, 0)),
        ],
        out_specs=pl.BlockSpec((members, 1, own, cols), lambda z: (0, z, 0, 0)),
        out_shape=jax.ShapeDtypeStruct((members, planes, own, cols), F32),
        scratch_shapes=[pltpu.VMEM((cols, rows), jnp.bfloat16)],
    )(score.T, event.T, leaf.T, local, base[None], columns)
    got = swap(parts.astype(jnp.float16), PLANE)
    plane_sum = jnp.sum(got.astype(F32), axis=0)
    got = swap(plane_sum.reshape(planes * cores, own // cores, cols), DEPTH_FEAT)
    summed = jnp.sum(got.reshape(planes, cores, own // cores, cols), axis=0)
    summed = summed * (BINS * LEAVES / (rows * shards) / DOWN)
    summed = summed.reshape(cores, BINS, 2, LEAVES, width)
    summed = jnp.moveaxis(summed, 0, 3).reshape(1, BINS, 2, LEAVES, cores * width)
    split_value = jnp.take(bins, split_feature, axis=1)
    new_leaf = 2 * leaf + (split_value > split_bin[None, :]).astype(jnp.int32)
    return (summed[:, :, 0], summed[:, :, 1], new_leaf)


def solution(mesh):
    finer = Mesh(
        mesh.devices.reshape(8, 4, 4, mesh.shape["feat"]), ("rows_0", "rows_1", "rows_2", "feat")
    )
    in_specs = (
        P(ROWS, "feat"),
        P(ROWS, "feat"),
        P(ROWS, "feat"),
        P(ROWS, None),
        P("feat"),
        P("feat"),
    )
    out_specs = (P(ROWS_FEAT, None, None, None), P(ROWS_FEAT, None, None, None), P(ROWS, "feat"))
    return jax.shard_map(
        per_device, mesh=finer, in_specs=in_specs, out_specs=out_specs, check_vma=False
    )
```

```python
import jax
import jax.numpy as jnp
from jax import lax
from jax.experimental import pallas as pl
from jax.experimental.pallas import tpu as pltpu
from jax.sharding import Mesh
from jax.sharding import PartitionSpec as P

BINS = 32
LEAVES = 2
AXES = ("far", "mate", "across", "down", "feat")
ROWS = AXES[:4]
PLANE = ("across", "down")
BLOCK = 256
F32 = jnp.float32
VMEM = 28 << 20
DOWN = 2.0**-3


def swap(x, axis):
    return lax.all_to_all(x, axis, split_axis=0, concat_axis=0, tiled=True)


def chosen_sum(got, here, earlier):
    index = lax.broadcasted_iota(jnp.int32, got.shape, 0)
    chosen = (index < here) if earlier else (index > here)
    return jnp.sum(jnp.where(chosen, got, 0.0), axis=0, keepdims=True)


def as_column(line):
    n = line.shape[1]
    row = lax.broadcasted_iota(jnp.int32, (n, n), 0)
    col = lax.broadcasted_iota(jnp.int32, (n, n), 1)
    return jnp.sum(jnp.where(row == col, jnp.broadcast_to(line, (n, n)), 0.0), axis=1, keepdims=True)


def as_line(column):
    n = column.shape[0]
    row = lax.broadcasted_iota(jnp.int32, (n, n), 0)
    col = lax.broadcasted_iota(jnp.int32, (n, n), 1)
    return jnp.sum(jnp.where(row == col, jnp.broadcast_to(column, (n, n)), 0.0), axis=0, keepdims=True)


def split_dot(x, ones):
    high = x.astype(jnp.bfloat16)
    rest = x - high.astype(F32)
    middle = rest.astype(jnp.bfloat16)
    low = (rest - middle.astype(F32)).astype(jnp.bfloat16)
    dot = lambda part: lax.dot(part, ones, preferred_element_type=F32)
    return (dot(low) + dot(middle)) + dot(high)


def total_kernel(score_ref, total_ref):
    total = jnp.sum(jnp.exp(score_ref[...]), axis=1, keepdims=True)
    total_ref[...] = jnp.broadcast_to(as_line(total), total_ref.shape)


def prefix_kernel(here_ref, score_ref, event_ref, later_ref, local_ref, total_ref):
    width, rows = score_ref.shape
    row = lax.broadcasted_iota(jnp.int32, (BLOCK, BLOCK), 0)
    col = lax.broadcasted_iota(jnp.int32, (BLOCK, BLOCK), 1)
    suffix = (row >= col).astype(F32).astype(jnp.bfloat16)
    prefix = (row <= col).astype(F32).astype(jnp.bfloat16)
    blocks = rows // BLOCK
    at = lambda k: pl.ds(k * BLOCK, BLOCK)
    e = jnp.concatenate([jnp.exp(score_ref[:, at(k)]) for k in range(blocks)], axis=0)
    runs = split_dot(e, suffix)
    carry = as_column(chosen_sum(later_ref[...], here_ref[0], False))
    both = [None] * blocks
    for k in reversed(range(blocks)):
        run = runs[k * width : (k + 1) * width]
        inverse = 1.0 / (run + carry)
        carry = carry + run[:, :1]
        share = event_ref[:, at(k)].astype(F32) * inverse
        both[k] = jnp.concatenate([share, share * inverse], axis=0)
    runs = split_dot(jnp.concatenate(both, axis=0), prefix)
    carry = jnp.zeros((2 * width, 1), F32)
    for k in range(blocks):
        run = runs[2 * k * width : 2 * (k + 1) * width]
        local_ref[:, at(k)] = run + carry
        carry = carry + run[:, BLOCK - 1 :]
    total_ref[...] = jnp.broadcast_to(as_line(carry), total_ref.shape)


def weigh_kernel(here_ref, base_ref, *refs):
    w_ref = refs[-1]
    for part in range(2):
        score_ref, event_ref, leaf_ref, local_ref = refs[4 * part : 4 * part + 4]
        width, rows = score_ref.shape
        base = as_column(chosen_sum(base_ref[...], here_ref[part], True))
        for k in range(rows // BLOCK):
            at = pl.ds(k * BLOCK, BLOCK)
            e = jnp.exp(score_ref[:, at])
            first = e * (local_ref[:width, at] + base[:width])
            second = e * e * (local_ref[width:, at] + base[width:])
            g = (first - event_ref[:, at].astype(F32)) * DOWN
            h = (first - second) * DOWN
            leaf = leaf_ref[:, at].astype(F32)
            for n, v in enumerate((g, h)):
                for m in range(LEAVES):
                    w_ref[
                        pl.ds((n * LEAVES + m) * width, width), pl.ds(part * rows + k * BLOCK, BLOCK)
                    ] = jnp.where(leaf == float(m), v, 0.0).astype(jnp.bfloat16)


def hist_kernel(w_ref, own_ref, mate_ref, out_ref):
    feats, rows = own_ref.shape
    level = lax.broadcasted_iota(jnp.int32, (BINS, 2 * rows), 0).astype(F32).astype(jnp.bfloat16)
    one = jnp.ones((), jnp.bfloat16)
    zero = jnp.zeros((), jnp.bfloat16)
    tiles = []
    for i in range(feats):
        line = jnp.concatenate([own_ref[pl.ds(i, 1), :], mate_ref[pl.ds(i, 1), :]], axis=1)
        line = jnp.broadcast_to(line, (BINS, 2 * rows)).astype(jnp.bfloat16)
        tiles.append(jnp.where(line == level, one, zero))
    hot = jnp.concatenate(tiles, axis=0)
    got = lax.dot_general(hot, w_ref[...], (((1,), (1,)), ((), ())), preferred_element_type=F32)
    out_ref[:, 0] = got.reshape(out_ref.shape[0], *out_ref.shape[2:])


def per_device(score, event, leaf, bins, split_feature, split_bin):
    rows, width = score.shape
    feats = bins.shape[1]
    shards = lax.axis_size(ROWS)
    cores = lax.axis_size("feat")
    cols = 2 * LEAVES * width
    far, mate, across, down = (lax.axis_size(a) for a in ROWS)
    members = across * down
    here = lax.axis_index(ROWS).astype(jnp.int32)
    both = jnp.stack([here, here ^ members])
    turned = both[::-1]
    scalar = pl.BlockSpec(memory_space=pltpu.SMEM)
    dense = pl.BlockSpec(memory_space=pltpu.VMEM)
    limit = pltpu.CompilerParams(vmem_limit_bytes=VMEM)
    pair = [(0, 1), (1, 0)]
    send = lambda x: lax.ppermute(x, "mate", pair)
    mate_score = send(score.T)
    copies = pl.pallas_call(
        total_kernel,
        out_shape=jax.ShapeDtypeStruct((shards, width), F32),
        compiler_params=limit,
    )(score.T)
    copies, score, event, leaf, bins = lax.optimization_barrier((copies, score, event, leaf, bins))
    totals = swap(copies, ROWS)
    columns = bins.T.astype(jnp.bfloat16).reshape(far, mate, -1, rows)
    side = lax.axis_index("mate")
    pick = lambda k: lax.dynamic_index_in_dim(columns, k, 1, keepdims=False).reshape(-1, rows)
    own_columns = pick(side).astype(F32)
    mate_event = send(event.T.astype(jnp.bfloat16))
    mate_columns = send(pick(1 - side))
    mate_leaf = send(leaf.T.astype(jnp.bfloat16))

    prefix = lambda order, s, e: pl.pallas_call(
        prefix_kernel,
        in_specs=[scalar, dense, dense, dense],
        out_shape=(
            jax.ShapeDtypeStruct((2 * width, rows), F32),
            jax.ShapeDtypeStruct((shards, 2 * width), F32),
        ),
        compiler_params=limit,
    )(order, s, e, totals)
    local, copies = prefix(both, score.T, event.T)
    base = swap(copies, ROWS)
    mate_local, _ = prefix(turned, mate_score, mate_event)
    weights = pl.pallas_call(
        weigh_kernel,
        in_specs=[scalar] + [dense] * 9,
        out_shape=jax.ShapeDtypeStruct((cols, 2 * rows), jnp.bfloat16),
        compiler_params=limit,
    )(both, base, score.T, event.T, leaf.T, local, mate_score, mate_event, mate_leaf, mate_local)
    own = cores * BINS
    step = members // 2
    slab = step * cores
    columns = pl.BlockSpec((slab, rows), lambda z, j: (2 * z + j, 0))
    parts = pl.pallas_call(
        hist_kernel,
        grid=(far, 2),
        in_specs=[pl.BlockSpec((cols, 2 * rows), lambda z, j: (0, 0)), columns, columns],
        out_specs=pl.BlockSpec((step, 1, own, cols), lambda z, j: (j, z, 0, 0)),
        out_shape=jax.ShapeDtypeStruct((members, far, own, cols), F32),
        compiler_params=limit,
    )(weights, own_columns, mate_columns.astype(F32))
    got = jnp.sum(swap(parts.astype(jnp.float16), PLANE).astype(F32), axis=0)
    got = swap(got.reshape(far * cores, BINS, cols), ("far", "feat"))
    summed = jnp.sum(got.reshape(far, cores, BINS, cols), axis=0)
    summed = summed * (BINS * LEAVES / (rows * shards) / DOWN)
    summed = summed.reshape(cores, BINS, 2, LEAVES, width)
    summed = jnp.moveaxis(summed, 0, 3).reshape(1, BINS, 2, LEAVES, cores * width)
    split_value = jnp.take(bins, split_feature, axis=1)
    new_leaf = 2 * leaf + (split_value > split_bin[None, :]).astype(jnp.int32)
    return (summed[:, :, 0], summed[:, :, 1], new_leaf)


def solution(mesh):
    finer = Mesh(
        mesh.devices.reshape(4, 2, 4, 4, mesh.shape["feat"]), AXES
    )
    in_specs = (
        P(ROWS, "feat"),
        P(ROWS, "feat"),
        P(ROWS, "feat"),
        P(ROWS, None),
        P("feat"),
        P("feat"),
    )
    out_specs = (P(AXES, None, None, None), P(AXES, None, None, None), P(ROWS, "feat"))
    return jax.shard_map(
        per_device, mesh=finer, in_specs=in_specs, out_specs=out_specs, check_vma=False
    )
```

```python
import jax
import jax.numpy as jnp
from jax import lax
from jax.experimental import pallas as pl
from jax.experimental.pallas import tpu as pltpu
from jax.sharding import Mesh
from jax.sharding import PartitionSpec as P


BINS = 32
LEAVES = 2
AXES = ("far", "mate", "across", "down", "feat")
ROWS = AXES[:4]
PLANE = ("across", "down")
BLOCK = 256
F32 = jnp.float32
VMEM = 28 << 20
DOWN = 2.0**-3


def swap(x, axis):
    return lax.all_to_all(x, axis, split_axis=0, concat_axis=0, tiled=True)


def chosen_sum(got, here, earlier):
    index = lax.broadcasted_iota(jnp.int32, got.shape, 0)
    chosen = (index < here) if earlier else (index > here)
    return jnp.sum(jnp.where(chosen, got, 0.0), axis=0, keepdims=True)


def as_column(line):
    n = line.shape[1]
    row = lax.broadcasted_iota(jnp.int32, (n, n), 0)
    col = lax.broadcasted_iota(jnp.int32, (n, n), 1)
    return jnp.sum(jnp.where(row == col, jnp.broadcast_to(line, (n, n)), 0.0), axis=1, keepdims=True)


def as_line(column):
    n = column.shape[0]
    row = lax.broadcasted_iota(jnp.int32, (n, n), 0)
    col = lax.broadcasted_iota(jnp.int32, (n, n), 1)
    return jnp.sum(jnp.where(row == col, jnp.broadcast_to(column, (n, n)), 0.0), axis=0, keepdims=True)


def split_dot(x, ones):
    high = x.astype(jnp.bfloat16)
    rest = x - high.astype(F32)
    middle = rest.astype(jnp.bfloat16)
    low = (rest - middle.astype(F32)).astype(jnp.bfloat16)
    dot = lambda part: lax.dot(part, ones, preferred_element_type=F32)
    return (dot(low) + dot(middle)) + dot(high)


def total_kernel(score_ref, total_ref):
    total = jnp.sum(jnp.exp(score_ref[...]), axis=1, keepdims=True)
    total_ref[...] = jnp.broadcast_to(as_line(total), total_ref.shape)


def hazards(here, score_ref, event_ref, later_ref):
    width, rows = score_ref.shape
    row = lax.broadcasted_iota(jnp.int32, (BLOCK, BLOCK), 0)
    col = lax.broadcasted_iota(jnp.int32, (BLOCK, BLOCK), 1)
    suffix = (row >= col).astype(F32).astype(jnp.bfloat16)
    blocks = rows // BLOCK
    at = lambda k: pl.ds(k * BLOCK, BLOCK)
    e = jnp.concatenate([jnp.exp(score_ref[:, at(k)]) for k in range(blocks)], axis=0)
    runs = split_dot(e, suffix)
    carry = as_column(chosen_sum(later_ref[...], here, False))
    both = [None] * blocks
    for k in reversed(range(blocks)):
        run = runs[k * width : (k + 1) * width]
        inverse = 1.0 / (run + carry)
        carry = carry + run[:, :1]
        share = event_ref[:, at(k)].astype(F32) * inverse
        both[k] = jnp.concatenate([share, share * inverse], axis=0)
    return e, both


def sums_kernel(here_ref, score_ref, event_ref, later_ref, total_ref):
    _, both = hazards(here_ref[0], score_ref, event_ref, later_ref)
    total = jnp.sum(sum(both[1:], both[0]), axis=1, keepdims=True)
    total_ref[...] = jnp.broadcast_to(as_line(total), total_ref.shape)


def local_kernel(here_ref, later_ref, *refs):
    out_ref = refs[-1]
    for part in range(2):
        score_ref, event_ref, leaf_ref = refs[3 * part : 3 * part + 3]
        width, rows = score_ref.shape
        e, both = hazards(here_ref[part], score_ref, event_ref, later_ref)
        row = lax.broadcasted_iota(jnp.int32, (BLOCK, BLOCK), 0)
        col = lax.broadcasted_iota(jnp.int32, (BLOCK, BLOCK), 1)
        prefix = (row <= col).astype(F32).astype(jnp.bfloat16)
        runs = split_dot(jnp.concatenate(both, axis=0), prefix)
        carry = jnp.zeros((2 * width, 1), F32)
        for k in range(rows // BLOCK):
            at = pl.ds(k * BLOCK, BLOCK)
            run = runs[2 * k * width : 2 * (k + 1) * width]
            here = run + carry
            carry = carry + run[:, BLOCK - 1 :]
            x = e[k * width : (k + 1) * width]
            product = x * here[:width]
            out_ref[3 * part, :, at] = product - event_ref[:, at].astype(F32)
            out_ref[3 * part + 1, :, at] = product - x * x * here[width:]
            out_ref[3 * part + 2, :, at] = jnp.where(leaf_ref[:, at].astype(F32) == 0.0, x, -x)


def weigh_kernel(here_ref, base_ref, held, w_ref):
    _, width, rows = held.shape
    for part in range(2):
        base = as_column(chosen_sum(base_ref[...], here_ref[part], True))
        for k in range(rows // BLOCK):
            at = pl.ds(k * BLOCK, BLOCK)
            signed = held[3 * part + 2, :, at]
            e = jnp.abs(signed)
            carried = e * base[:width]
            g = (held[3 * part, :, at] + carried) * DOWN
            h = (held[3 * part + 1, :, at] + (carried - e * e * base[width:])) * DOWN
            for n, v in enumerate((g, h)):
                for m in range(LEAVES):
                    keep = (signed < 0.0) if m else (signed > 0.0)
                    w_ref[
                        pl.ds((n * LEAVES + m) * width, width), pl.ds(part * rows + k * BLOCK, BLOCK)
                    ] = jnp.where(keep, v, 0.0).astype(jnp.bfloat16)


def hist_kernel(w_ref, own_ref, mate_ref, out_ref, line_ref):
    feats, rows = own_ref.shape
    line_ref[:, :rows] = own_ref[...].astype(F32)
    line_ref[:, rows:] = mate_ref[...].astype(F32)
    level = lax.broadcasted_iota(jnp.int32, (BINS, 2 * rows), 0).astype(F32).astype(jnp.bfloat16)
    one = jnp.ones((), jnp.bfloat16)
    zero = jnp.zeros((), jnp.bfloat16)
    tiles = []
    for i in range(feats):
        line = jnp.broadcast_to(line_ref[pl.ds(i, 1), :], (BINS, 2 * rows)).astype(jnp.bfloat16)
        tiles.append(jnp.where(line == level, one, zero))
    hot = jnp.concatenate(tiles, axis=0)
    got = lax.dot_general(hot, w_ref[...], (((1,), (1,)), ((), ())), preferred_element_type=F32)
    out_ref[:, 0] = got.reshape(out_ref.shape[0], *out_ref.shape[2:])


def per_device(score, event, leaf, bins, split_feature, split_bin):
    rows, width = score.shape
    shards = lax.axis_size(ROWS)
    cores = lax.axis_size("feat")
    cols = 2 * LEAVES * width
    far, mate, across, down = (lax.axis_size(a) for a in ROWS)
    members = across * down
    here = lax.axis_index(ROWS).astype(jnp.int32)
    both = jnp.stack([here, here ^ members])
    scalar = pl.BlockSpec(memory_space=pltpu.SMEM)
    dense = pl.BlockSpec(memory_space=pltpu.VMEM)
    limit = pltpu.CompilerParams(vmem_limit_bytes=VMEM)
    pair = [(0, 1), (1, 0)]
    send = lambda x: lax.ppermute(x, "mate", pair)
    mate_score = send(score.T)
    copies = pl.pallas_call(
        total_kernel,
        out_shape=jax.ShapeDtypeStruct((shards, width), F32),
        compiler_params=limit,
    )(score.T)
    copies, score, event, leaf, bins = lax.optimization_barrier((copies, score, event, leaf, bins))
    totals = swap(copies, ROWS)
    columns = bins.T.astype(jnp.bfloat16).reshape(far, mate, -1, rows)
    side = lax.axis_index("mate")
    pick = lambda k: lax.dynamic_index_in_dim(columns, k, 1, keepdims=False).reshape(-1, rows)
    own_columns = pick(side)
    mate_event = send(event.T.astype(jnp.bfloat16))
    mate_columns = send(pick(1 - side))
    mate_leaf = send(leaf.T.astype(jnp.bfloat16))

    copies = pl.pallas_call(
        sums_kernel,
        in_specs=[scalar, dense, dense, dense],
        out_shape=jax.ShapeDtypeStruct((shards, 2 * width), F32),
        compiler_params=limit,
    )(both, score.T, event.T, totals)
    copies, split_feature, routed = lax.optimization_barrier((copies, split_feature, leaf))
    base = swap(copies, ROWS)
    split_value = jnp.take(bins, split_feature, axis=1)
    new_leaf = 2 * routed + (split_value > split_bin[None, :]).astype(jnp.int32)
    base, new_leaf = lax.optimization_barrier((base, new_leaf))
    locals_ = pl.pallas_call(
        local_kernel,
        in_specs=[scalar] + [dense] * 7,
        out_shape=jax.ShapeDtypeStruct((6, width, rows), F32),
    )(both, totals, score.T, event.T, leaf.T, mate_score, mate_event, mate_leaf)
    weights = pl.pallas_call(
        weigh_kernel,
        in_specs=[scalar, dense, dense],
        out_shape=jax.ShapeDtypeStruct((cols, 2 * rows), jnp.bfloat16),
        compiler_params=limit,
    )(both, base, locals_)
    own = cores * BINS
    step = members // 2
    slab = step * cores
    columns = pl.BlockSpec((slab, rows), lambda z, j: (2 * z + j, 0))
    parts = pl.pallas_call(
        hist_kernel,
        grid=(far, 2),
        in_specs=[pl.BlockSpec((cols, 2 * rows), lambda z, j: (0, 0)), columns, columns],
        out_specs=pl.BlockSpec((step, 1, own, cols), lambda z, j: (j, z, 0, 0)),
        out_shape=jax.ShapeDtypeStruct((members, far, own, cols), F32),
        scratch_shapes=[pltpu.VMEM((slab, 2 * rows), F32)],
        compiler_params=limit,
    )(weights, own_columns, mate_columns)
    got = jnp.sum(swap(parts.astype(jnp.float16), PLANE).astype(F32), axis=0)
    got = swap(got.reshape(far * cores, BINS, cols), ("far", "feat"))
    summed = jnp.sum(got.reshape(far, cores, BINS, cols), axis=0)
    summed = summed * (BINS * LEAVES / (rows * shards) / DOWN)
    summed = summed.reshape(cores, BINS, 2, LEAVES, width)
    summed = jnp.moveaxis(summed, 0, 3).reshape(1, BINS, 2, LEAVES, cores * width)
    return (summed[:, :, 0], summed[:, :, 1], new_leaf)


def solution(mesh):
    finer = Mesh(
        mesh.devices.reshape(4, 2, 4, 4, mesh.shape["feat"]), AXES
    )
    in_specs = (
        P(ROWS, "feat"),
        P(ROWS, "feat"),
        P(ROWS, "feat"),
        P(ROWS, None),
        P("feat"),
        P("feat"),
    )
    out_specs = (P(AXES, None, None, None), P(AXES, None, None, None), P(ROWS, "feat"))
    return jax.shard_map(per_device, mesh=finer, in_specs=in_specs, out_specs=out_specs, check_vma=False)
```
